16 devices in a mesh: dp: 2 (over y, z), tp: 8 (over x, core).
Axes of the slice: x: 4, y: 2, z: 1, core: 2. Of those that a mesh axis runs over, the one named last changes fastest.
The devices are a block of a 4x4x8 slice.
Arguments:
- x: bfloat16 [2, 2048, 5120], P('dp', 'tp'), parts along dimension 0
- dy: bfloat16 [2, 2048, 5120], P('dp', 'tp'), parts along dimension 0
- wq: bfloat16 [5120, 5120], P(None, 'tp')
- wk: bfloat16 [5120, 1024], P(None, 'tp')
- wv: bfloat16 [5120, 1024], P(None, 'tp')
- wo: bfloat16 [5120, 5120], P('tp')
- w_gate: bfloat16 [5120, 17408], P(None, 'tp')
- w_up: bfloat16 [5120, 17408], P(None, 'tp')
- w_down: bfloat16 [17408, 5120], P('tp')
Outputs:
- output 1: bfloat16 [2, 2048, 5120], P('dp', 'tp'), parts along dimension 0
- output 2: bfloat16 [10240, 5120], P('dp', 'tp'), parts along dimension 0
- output 3: bfloat16 [10240, 1024], P('dp', 'tp'), parts along dimension 0
- output 4: bfloat16 [10240, 1024], P('dp', 'tp'), parts along dimension 0
- output 5: bfloat16 [10240, 5120], P(('dp', 'tp')), parts along dimension 0
- output 6: bfloat16 [10240, 17408], P('dp', 'tp'), parts along dimension 0
- output 7: bfloat16 [10240, 17408], P('dp', 'tp'), parts along dimension 0
- output 8: bfloat16 [34816, 5120], P(('dp', 'tp')), parts along dimension 0
There are 2 independent parts. The reference program is written for one: setup_inputs(seed, part) draws one part's arguments, and reference() takes and returns one part's arrays. A program takes and returns all parts, laid end to end along the dimension named above; an argument that names none is the same for every part.
All inputs are finite; a program needn't handle non-finite values.
Results may differ from the reference program's by a relative error of at most 0.024.
Values are sent between devices in bfloat16 or wider.
A program may use at most 768 MiB of HBM per device.

```python
import jax
import jax.numpy as jnp
from jax import lax

SEQUENCES = 1
TOKENS = 2048
D = 5120
HEADS = 40
KV_HEADS = 8
HEAD = 128
FF = 17408
THETA = 10000
NAMES = ("wq", "wk", "wv", "wo", "w_gate", "w_up", "w_down")
SHAPES = {
    "wq": (D, HEADS * HEAD),
    "wk": (D, KV_HEADS * HEAD),
    "wv": (D, KV_HEADS * HEAD),
    "wo": (HEADS * HEAD, D),
    "w_gate": (D, FF),
    "w_up": (D, FF),
    "w_down": (FF, D),
}


def bump(key, n, height):
    away = (jnp.arange(n, dtype=jnp.int32) - jax.random.randint(key, (), 0, n, jnp.int32)) % n
    return jnp.where(away < n // 8, height, 1.0)


def together(key, own, strength):
    shared = jax.random.normal(key, own.shape[1:], jnp.float32)
    return (own + strength * shared) * lax.rsqrt(1 + strength * strength)


def setup_inputs(seed: int = 0, part: int = 0) -> dict:
    kx, kdy, ka, kb, kz, kf, kh, kl, *kw = jax.random.split(jax.random.key(seed), 8 + len(NAMES))
    kx, kdy, ka, kb = (jax.random.fold_in(k, part) for k in (kx, kdy, ka, kb))
    shape = (SEQUENCES, TOKENS, D)
    much_x, much_dy = jax.random.uniform(kz, (2,), jnp.float32, 0.0, 1.0)
    loud = 2.0 ** jax.random.uniform(jax.random.fold_in(kz, 1), (), jnp.float32, -1.0, 2.0)
    halves = 2.0 ** jax.random.uniform(kl, (2,), jnp.float32, -1.0, 1.0)
    times = {"wq": 1.0, "wk": 1.0, "wv": 2.0, "wo": halves[0], "w_gate": 1.0, "w_up": bump(kh, FF, 4.0), "w_down": halves[1]}
    x = together(ka, jax.random.normal(kx, shape, jnp.float32), much_x) * bump(kf, D, 4.0)
    dy = together(kb, jax.random.normal(kdy, shape, jnp.float32), much_dy)
    drawn = {"x": x.astype(jnp.bfloat16), "dy": (loud * dy * (SEQUENCES * TOKENS) ** -0.5).astype(jnp.bfloat16)}
    for key, name in zip(kw, NAMES, strict=True):
        drawn[name] = (jax.random.normal(key, SHAPES[name], jnp.float32) * SHAPES[name][0] ** -0.5 * times[name]).astype(jnp.bfloat16)
    return drawn


def matmul(a, w):
    return jnp.dot(a, w, preferred_element_type=jnp.float32).astype(jnp.bfloat16)


def normed(h):
    wide = h.astype(jnp.float32)
    scale = lax.rsqrt(jnp.mean(wide**2, -1, keepdims=True) + 1e-6)
    return (wide * scale).astype(jnp.bfloat16)


def turned(t, theta):
    half = t.shape[-1] // 2
    angle = jnp.arange(t.shape[0], dtype=jnp.float32)[:, None] * theta ** (-jnp.arange(half, dtype=jnp.float32) / half)
    cos, sin = jnp.cos(angle)[:, None], jnp.sin(angle)[:, None]
    a, b = t[..., :half].astype(jnp.float32), t[..., half:].astype(jnp.float32)
    return jnp.concatenate([a * cos - b * sin, b * cos + a * sin], -1).astype(jnp.bfloat16)


def seen_by(q, k, v):
    tokens, kv = q.shape[0], k.shape[1]
    q = q.reshape(tokens, kv, -1, q.shape[-1])
    scores = jnp.einsum("tgsd,ugd->gstu", q.astype(jnp.float32), k.astype(jnp.float32)) * q.shape[-1] ** -0.5
    place = jnp.arange(tokens)
    weights = jax.nn.softmax(jnp.where(place[:, None] >= place, scores, -jnp.inf), -1).astype(jnp.bfloat16)
    return jnp.einsum("gstu,ugd->tgsd", weights.astype(jnp.float32), v.astype(jnp.float32)).astype(jnp.bfloat16).reshape(tokens, -1)


def layer(h, w):
    a = normed(h)
    q, k = (turned(matmul(a, w[name]).reshape(h.shape[0], -1, HEAD), THETA) for name in ("wq", "wk"))
    h = h + matmul(seen_by(q, k, matmul(a, w["wv"]).reshape(h.shape[0], -1, HEAD)), w["wo"])
    b = normed(h)
    gate = jnp.dot(b, w["w_gate"], preferred_element_type=jnp.float32)
    up = jnp.dot(b, w["w_up"], preferred_element_type=jnp.float32)
    return h + matmul((jax.nn.silu(gate) * up).astype(jnp.bfloat16), w["w_down"])


def reference(x, dy, wq, wk, wv, wo, w_gate, w_up, w_down):
    weights = dict(zip(NAMES, (wq, wk, wv, wo, w_gate, w_up, w_down), strict=True))

    def take(so_far, sequence):
        h, by_y = sequence
        _, back = jax.vjp(lambda w, h: layer(h, w), weights, h)
        by_weights, by_h = back(by_y)
        return jax.tree.map(lambda total, term: total + term.astype(jnp.float32), so_far, by_weights), by_h

    none_yet = {name: jnp.zeros(w.shape, jnp.float32) for name, w in weights.items()}
    by_weights, by_x = lax.scan(take, none_yet, (x, dy))
    return (by_x, *(by_weights[name].astype(jnp.bfloat16) for name in NAMES))
```

```python
import functools

import jax
import jax.numpy as jnp
from jax import lax
from jax.experimental import pallas as pl
from jax.experimental.pallas import tpu as pltpu

NEG = -1e30
HIDDEN = 2 * NEG
LOG2E = 1.4426950408889634
VMEM = 56 * 2**20
STRIP = 512


def _fit(size, want, unit=128):
    return max(n for n in range(unit, max(min(want, size), unit) + 1, unit) if size % n == 0)


def _dot(a, b, ca, cb):
    return lax.dot_general(a, b, (((ca,), (cb,)), ((), ())), preferred_element_type=jnp.float32)


def _gap(bk, cols, bq):
    return lax.rem(lax.broadcasted_iota(jnp.int32, (bk, cols), 1), bq) - lax.broadcasted_iota(jnp.int32, (bk, cols), 0)


def _row(ref):
    return jnp.concatenate([ref[n : n + 1, :] for n in range(ref.shape[0])], axis=1)


def _blocks(block, iq, bq, bk):
    whole, last = lax.div(iq * bq + 1, bk), lax.div(iq * bq + bq - 1 + bk, bk)
    lax.fori_loop(0, whole, lambda j, _: block(j, False), None)
    lax.fori_loop(whole, last, lambda j, _: block(j, True), None)


def _forward(q_ref, k_ref, v_ref, o_ref, lse_ref, top_s, mix_s, gap_s, *, scale, bq, bk):
    g, _, d = q_ref.shape
    low, cols = k_ref.dtype, g * bq
    iq = pl.program_id(0)
    e = scale * LOG2E
    wide = _fit(cols, STRIP)
    strips = range(0, cols, wide)
    gap_s[...] = _gap(bk, cols, bq)
    top_s[...] = jnp.full_like(top_s, NEG)
    mix_s[...] = jnp.zeros_like(mix_s)
    ones = jnp.ones((8, bk), low)

    def block(j, masked):
        here = pl.ds(j * bk, bk)
        scores = [_dot(k_ref[0, here, :], q_ref[...].reshape(cols, d)[at : at + wide, :], 1, 1) for at in strips]
        weights, keeps = [], []
        for at, s in zip(strips, scores):
            if masked:
                s = jnp.where(gap_s[:, at : at + wide] >= j * bk - iq * bq, s, HIDDEN)
            old = top_s[:, at : at + wide]
            top = jnp.maximum(old, s.max(axis=0, keepdims=True))
            top_s[:, at : at + wide] = top
            weights.append(jnp.exp2((s - top) * e).astype(low))
            keeps.append(jnp.exp2((old - top) * e))
        for at, p, keep in zip(strips, weights, keeps):
            values = jnp.concatenate([v_ref[0, here, :].T, ones], axis=0)
            mix_s[:, at : at + wide] = mix_s[:, at : at + wide] * keep + _dot(values, p, 1, 0)

    _blocks(block, iq, bq, bk)
    total = mix_s[d : d + 1, :]
    o_ref[...] = (mix_s[:d, :] * (1 / total)).T.reshape(g, bq, d).astype(low)
    lse = top_s[...] * scale + jnp.log(total)
    for n in range(g):
        lse_ref[n : n + 1, :] = lse[:, n * bq : (n + 1) * bq]


def _backward(q_ref, k_ref, v_ref, do_ref, o_ref, lse_ref, cos_ref, sin_ref, dq_ref, dk_ref, dv_ref, dq_s, dk_s, dv_s, gap_s, *, scale, bq, bk):
    g, _, d = q_ref.shape
    low, cols = q_ref.dtype, g * bq
    iq = pl.program_id(0)
    e = scale * LOG2E
    wide = _fit(cols, STRIP)
    strips = range(0, cols, wide)

    @pl.when(iq == 0)
    def _():
        gap_s[...] = _gap(bk, cols, bq)
        dk_s[...] = jnp.zeros_like(dk_s)
        dv_s[...] = jnp.zeros_like(dv_s)

    dq_s[...] = jnp.zeros_like(dq_s)
    lses = _row(lse_ref) * LOG2E
    deltas = (do_ref[...].reshape(cols, d).astype(jnp.float32) * o_ref[...].reshape(cols, d).astype(jnp.float32)).T.sum(axis=0, keepdims=True)

    def block(j, masked):
        here = pl.ds(j * bk, bk)
        qs = [q_ref[...].reshape(cols, d)[at : at + wide, :] for at in strips]
        dos = [do_ref[...].reshape(cols, d)[at : at + wide, :] for at in strips]
        scores = [_dot(k_ref[0, here, :], x, 1, 1) for x in qs]
        dps = [_dot(v_ref[0, here, :], x, 1, 1) for x in dos]
        for n, at in enumerate(strips):
            p = jnp.exp2(scores[n] * e - lses[:, at : at + wide])
            if masked:
                p = jnp.where(gap_s[:, at : at + wide] >= j * bk - iq * bq, p, 0.0)
            ds = (p * (dps[n] - deltas[:, at : at + wide])).astype(low)
            dv_s[here, :] += _dot(p.astype(low), dos[n], 1, 0)
            dk_s[here, :] += _dot(ds, qs[n], 1, 0)
            dq_s[:, at : at + wide] += _dot(k_ref[0, here, :].T, ds, 1, 0)

    _blocks(block, iq, bq, bk)
    here = pl.ds(iq * bq, bq)
    for n in range(g):
        part = (dq_s[:, n * bq : (n + 1) * bq] * scale).T.astype(low)
        dq_ref[:, n * d : (n + 1) * d] = turned(part, cos_ref[here, :], -sin_ref[here, :])

    @pl.when(iq == pl.num_programs(0) - 1)
    def _():
        dk_ref[...] = turned((dk_s[...] * scale).astype(low), cos_ref[...], -sin_ref[...])
        dv_ref[...] = dv_s[...].astype(low)


def _attention(body, q, specs, args, out_specs, outs, scratch, width, bq, bk):
    g, tokens, d = q.shape
    shapes = [jax.ShapeDtypeStruct(*o) for o in outs]
    return pl.pallas_call(
        functools.partial(body, scale=d**-0.5, bq=bq, bk=bk),
        grid=(tokens // bq,),
        in_specs=specs,
        out_specs=out_specs,
        scratch_shapes=[pltpu.VMEM(*t) for t in scratch],
        out_shape=shapes,
        compiler_params=pltpu.CompilerParams(dimension_semantics=("arbitrary",), vmem_limit_bytes=VMEM),
        cost_estimate=pl.CostEstimate(flops=width * g * tokens * tokens * d, transcendentals=g * tokens * tokens,
                                      bytes_accessed=sum(a.size * a.dtype.itemsize for a in [*args, *shapes])),
    )(*args)


def attend(q, k, v, bq=768, bk=512):
    g, tokens, d = q.shape
    bq, bk = _fit(tokens, bq), _fit(tokens, bk)
    queries = pl.BlockSpec((g, bq, d), lambda i: (0, i, 0))
    keys = pl.BlockSpec((1, tokens, d), lambda i: (0, 0, 0))
    return _attention(_forward, q, [queries, keys, keys], (q, k, v), [queries, pl.BlockSpec((g, bq), lambda i: (0, i))],
                      [(q.shape, q.dtype), ((g, tokens), jnp.float32)],
                      [((1, g * bq), jnp.float32), ((d + 8, g * bq), jnp.float32), ((bk, g * bq), jnp.int32)], 2, bq, bk)


def attend_back(q, k, v, do, out, lse, cos, sin, bq=256, bk=512):
    g, tokens, d = q.shape
    bq, bk = _fit(tokens, bq), _fit(tokens, bk)
    queries = pl.BlockSpec((g, bq, d), lambda i: (0, i, 0))
    keys = pl.BlockSpec((1, tokens, d), lambda i: (0, 0, 0))
    flat = pl.BlockSpec((tokens, d), lambda i: (0, 0))
    return _attention(_backward, q, [queries, keys, keys, queries, queries, pl.BlockSpec((g, bq), lambda i: (0, i)), flat, flat],
                      (q, k, v, do, out, lse, cos, sin), [pl.BlockSpec((bq, g * d), lambda i: (i, 0)), flat, flat],
                      [((tokens, n * d), q.dtype) for n in (g, 1, 1)],
                      [((d, g * bq), jnp.float32), ((tokens, d), jnp.float32), ((tokens, d), jnp.float32), ((bk, g * bq), jnp.int32)], 5, bq, bk)


from jax.sharding import PartitionSpec as P


HEAD = 128
THETA = 10000
ROOM = 63 * 2**20
BF16, F32 = jnp.bfloat16, jnp.float32
PIECES = 2


def nn(a, b):
    return jnp.dot(a, b, preferred_element_type=F32)


def nt(a, b):
    return lax.dot_general(a, b, (((1,), (1,)), ((), ())), preferred_element_type=F32)


def tn(a, b):
    return lax.dot_general(a, b, (((0,), (0,)), ((), ())), preferred_element_type=F32)


def whole(*shape):
    return pl.BlockSpec(shape, lambda *_: (0,) * len(shape), pipeline_mode=pl.Buffered(1))


def run(body, grid, in_specs, out_specs, outs, args, flops, scratch=()):
    out_shape = [jax.ShapeDtypeStruct(s, t) for s, t in outs]
    moved = sum(a.size * a.dtype.itemsize for a in [*args, *out_shape])
    return pl.pallas_call(
        body,
        grid=grid,
        in_specs=in_specs,
        out_specs=out_specs,
        out_shape=out_shape,
        scratch_shapes=list(scratch),
        compiler_params=pltpu.CompilerParams(vmem_limit_bytes=ROOM, dimension_semantics=("arbitrary",) * len(grid)),
        cost_estimate=pl.CostEstimate(flops=flops, bytes_accessed=moved, transcendentals=0),
    )(*args)


def scale_of(wide):
    return lax.rsqrt(jnp.mean(wide**2, -1, keepdims=True) + 1e-6)


def normed(x):
    rows, d = x.shape
    tall = _fit(rows, 64, 16)

    def body(x_ref, a_ref):
        wide = x_ref[...].astype(F32)
        a_ref[...] = (wide * scale_of(wide)).astype(BF16)

    block = pl.BlockSpec((tall, d), lambda i: (i, 0))
    return run(body, (rows // tall,), [block], [block], [((rows, d), BF16)], (x,), 8 * rows * d)[0]


def added(x, term, piece):
    rows, d = term.shape
    tall = _fit(rows, 32, 16)
    steps = rows // tall

    def body(x_ref, t_ref, h_ref, b_ref):
        h = x_ref[...] + t_ref[...]
        wide = h.astype(F32)
        h_ref[...] = h
        b_ref[...] = (wide * scale_of(wide)).astype(BF16)

    block = pl.BlockSpec((tall, d), lambda i: (i, 0))
    return run(body, (steps,), [pl.BlockSpec((tall, d), lambda i: (piece * steps + i, 0)), block], [block] * 2, [((rows, d), BF16)] * 2,
               (x, term), 8 * rows * d)


def back_through_norm(h, by):
    wide, by = h.astype(F32), by.astype(F32)
    scale = scale_of(wide)
    return (by * scale - wide * (scale**3 * jnp.mean(by * wide, -1, keepdims=True))).astype(BF16)


def by_states(dy, h, by, piece):
    rows, d = h.shape
    tall = _fit(rows, 32, 16)
    steps = rows // tall

    def body(dy_ref, h_ref, by_ref, o_ref):
        o_ref[...] = dy_ref[...] + back_through_norm(h_ref[...], by_ref[...])

    block = pl.BlockSpec((tall, d), lambda i: (i, 0))
    return run(body, (steps,), [pl.BlockSpec((tall, d), lambda i: (piece * steps + i, 0)), block, block], [block], [((rows, d), BF16)],
               (dy, h, by), 12 * rows * d)[0]


def by_x(dhs, x, das):
    tokens, d = x.shape
    rows = tokens // PIECES
    tall = _fit(rows, 32, 16)
    steps = rows // tall

    def body(x_ref, *refs):
        for c in range(PIECES):

            @pl.when(pl.program_id(0) // steps == c)
            def _():
                refs[-1][...] = refs[c][...] + back_through_norm(x_ref[...], refs[PIECES + c][...])

    block = pl.BlockSpec((tall, d), lambda i: (i, 0))
    piece = lambda c: pl.BlockSpec((tall, d), lambda i: (jnp.clip(i - c * steps, 0, steps - 1), 0))
    return run(body, (PIECES * steps,), [block] + [piece(c) for c in range(PIECES)] * 2, [block], [((tokens, d), BF16)], (x, *dhs, *das),
               12 * tokens * d)[0]


def tables(tokens):
    half = HEAD // 2
    angle = jnp.arange(tokens, dtype=F32)[:, None] * THETA ** (-jnp.arange(half, dtype=F32) / half)
    cos, sin = jnp.cos(angle), jnp.sin(angle)
    return jnp.concatenate([cos, cos], 1), jnp.concatenate([-sin, sin], 1)


def turned(t, cos, sin):
    t = t.astype(F32)
    return (t * cos + pltpu.roll(t, HEAD // 2, 1) * sin).astype(BF16)


def qkv(a, wq, wk, wv, cos, sin):
    tokens, d = a.shape
    n, kv = wq.shape[1] // HEAD, wk.shape[1] // HEAD
    rows = _fit(tokens, 512)

    def body(a_ref, wq_ref, wk_ref, wv_ref, cos_ref, sin_ref, q_ref, k_ref, v_ref):
        c, s = cos_ref[...], sin_ref[...]
        q = nn(a_ref[...], wq_ref[...]).astype(BF16)
        for i in range(n):
            q_ref[i] = turned(q[:, i * HEAD : (i + 1) * HEAD], c, s)
        both = nn(a_ref[...], jnp.concatenate([wk_ref[...], wv_ref[...]], axis=1)).astype(BF16)
        for i in range(kv):
            k_ref[i] = turned(both[:, i * HEAD : (i + 1) * HEAD], c, s)
            v_ref[i] = both[:, (kv + i) * HEAD : (kv + i + 1) * HEAD]

    block = pl.BlockSpec((rows, d), lambda i: (i, 0))
    table = pl.BlockSpec((rows, HEAD), lambda i: (i, 0))
    by_head = lambda m: pl.BlockSpec((m, rows, HEAD), lambda i: (0, i, 0))
    return run(body, (tokens // rows,), [block, whole(*wq.shape), whole(*wk.shape), whole(*wv.shape), table, table],
               [by_head(n), by_head(kv), by_head(kv)], [((m, tokens, HEAD), BF16) for m in (n, kv, kv)], (a, wq, wk, wv, cos, sin),
               2 * tokens * d * (n + 2 * kv) * HEAD)


def projected(heads, wo, tp, piece):
    n, tokens, _ = heads.shape
    d = wo.shape[1]
    each = tokens // tp // PIECES
    wide = _fit(d, 1024)

    def body(h_ref, w_ref, o_ref):
        h = jnp.concatenate([h_ref[i].reshape(tp * each, HEAD) for i in range(n)], axis=1)
        o_ref[...] = nn(h, w_ref[...]).astype(BF16)

    return run(body, (d // wide,),
               [pl.BlockSpec((n, tp, None, each, HEAD), lambda j: (0, 0, piece, 0, 0)), pl.BlockSpec((n * HEAD, wide), lambda j: (0, j))],
               [pl.BlockSpec((tp * each, wide), lambda j: (0, j))], [((tp * each, d), BF16)],
               (heads.reshape(n, tp, PIECES, each, HEAD), wo), 2 * tp * each * n * HEAD * d)[0]


def by_hidden(dy, wd):
    tokens, d = dy.shape
    ff = wd.shape[0]
    rows, wide = _fit(tokens, 1024), 256

    def body(dy_ref, w_ref, o_ref):
        o_ref[...] = nt(dy_ref[...], w_ref[...]).astype(BF16)

    return run(body, (tokens // rows, pl.cdiv(ff, wide)),
               [pl.BlockSpec((rows, d), lambda i, j: (i, 0)), pl.BlockSpec((wide, d), lambda i, j: (j, 0))],
               [pl.BlockSpec((rows, wide), lambda i, j: (i, j))], [((tokens, ff), BF16)], (dy, wd), 2 * tokens * d * ff)[0]


def gated(b, wg, wu, dhid, tp, piece):
    rows, d = b.shape
    ff = wg.shape[1]
    each = rows // tp

    def body(b_ref, wg_ref, wu_ref, dh_ref, h_ref, dg_ref, du_ref):
        y = nn(b_ref[...], jnp.concatenate([wg_ref[...], wu_ref[...]], axis=1))
        gate, up, by = y[:, :128], y[:, 128:], dh_ref[...].reshape(rows, 128).astype(F32)
        s = jax.nn.sigmoid(gate)
        silu = gate * s
        h_ref[...] = (silu * up).astype(BF16)
        dg_ref[...] = (by * up * (s * (1 + gate * (1 - s)))).astype(BF16)
        du_ref[...] = (by * silu).astype(BF16)

    w, out = pl.BlockSpec((d, 128), lambda j: (0, j)), pl.BlockSpec((rows, 128), lambda j: (0, j))
    return run(body, (ff // 128,), [whole(rows, d), w, w, pl.BlockSpec((tp, None, each, 128), lambda j: (0, piece, 0, j))],
               [out] * 3, [((rows, ff), BF16)] * 3, (b, wg, wu, dhid.reshape(tp, PIECES, each, ff)), 4 * rows * d * ff)


def by_normed(dg, du, wg, wu):
    rows, ff = dg.shape
    d = wg.shape[0]
    wide = _fit(d, 512)

    def body(dg_ref, du_ref, wg_ref, wu_ref, o_ref):
        o_ref[...] = nt(jnp.concatenate([dg_ref[...], du_ref[...]], axis=1), jnp.concatenate([wg_ref[...], wu_ref[...]], axis=1)).astype(BF16)

    w = pl.BlockSpec((wide, ff), lambda j: (j, 0))
    return run(body, (d // wide,), [whole(rows, ff), whole(rows, ff), w, w], [pl.BlockSpec((rows, wide), lambda j: (0, j))],
               [((rows, d), BF16)], (dg, du, wg, wu), 4 * rows * d * ff)[0]


def by_columns(bs, ds):
    n, (rows, d), ff = len(bs), bs[0].shape, ds[0].shape[1]
    tall = _fit(d, 512)

    def body(*refs):
        refs[-1][...] = sum(nn(b[...].T, r[...]) for b, r in zip(refs[:n], refs[n : 2 * n])).astype(BF16)

    return run(body, (d // tall,), [pl.BlockSpec((rows, tall), lambda i: (0, i))] * n + [whole(rows, ff)] * n,
               [pl.BlockSpec((tall, ff), lambda i: (i, 0))], [((d, ff), BF16)], (*bs, *ds), 2 * n * rows * d * ff)[0]


def by_down(hids, dy, tp):
    n, (rows, ff), d = len(hids), hids[0].shape, dy.shape[1]
    each, wide = rows // tp, _fit(d, 512)

    def body(*refs):
        h, (dy_ref, o_ref) = refs[:n], refs[n:]
        o_ref[...] = sum(tn(r[...], dy_ref[:, c].reshape(rows, wide)) for c, r in enumerate(h)).astype(BF16)

    return run(body, (d // wide,), [whole(rows, ff)] * n + [pl.BlockSpec((tp, n, each, wide), lambda j: (0, 0, 0, j))],
               [pl.BlockSpec((ff, wide), lambda j: (0, j))], [((ff, d), BF16)], (*hids, dy.reshape(tp, n, each, d)), 2 * n * rows * d * ff)[0]


def by_heads(dhs, wo, n, tp):
    rows, d = dhs[0].shape
    each = rows // tp
    some = _fit(tp, max(512 // each, 1), 1)
    steps = tp // some

    def body(*refs):
        w_ref, do_ref = refs[PIECES:]
        for c in range(PIECES):

            @pl.when(pl.program_id(0) // steps == c)
            def _():
                y = nt(refs[c][...], w_ref[...]).astype(BF16)
                for i in range(n):
                    do_ref[i] = y[:, i * HEAD : (i + 1) * HEAD].reshape(some, each, HEAD)

    piece = lambda c: pl.BlockSpec((some * each, d), lambda i: (jnp.clip(i - c * steps, 0, steps - 1), 0))
    return run(body, (PIECES * steps,), [piece(c) for c in range(PIECES)] + [whole(*wo.shape)],
               [pl.BlockSpec((n, some, None, each, HEAD), lambda i: (0, i % steps, i // steps, 0, 0))],
               [((n, tp, PIECES, each, HEAD), BF16)], (*dhs, wo), 2 * PIECES * rows * d * n * HEAD)[0].reshape(n, PIECES * rows, HEAD)


def by_wo(heads, dhs, tp):
    n = heads.shape[0]
    rows, d = dhs[0].shape
    each, wide = rows // tp, _fit(d, 512)

    def body(h_ref, *refs):
        dh, o_ref = refs[:PIECES], refs[PIECES]
        left = lambda c: jnp.concatenate([h_ref[i, :, c].reshape(rows, HEAD) for i in range(n)], axis=1)
        o_ref[...] = sum(tn(left(c), dh[c][...]) for c in range(PIECES)).astype(BF16)

    return run(body, (d // wide,), [whole(n, tp, PIECES, each, HEAD)] + [pl.BlockSpec((rows, wide), lambda j: (0, j))] * PIECES,
               [pl.BlockSpec((n * HEAD, wide), lambda j: (0, j))], [((n * HEAD, d), BF16)], (heads.reshape(n, tp, PIECES, each, HEAD), *dhs),
               2 * PIECES * rows * d * n * HEAD)[0]


def by_input(dq, dk, dv, wq, wk, wv, tp, piece):
    tokens, nq = dq.shape
    nk, d = dk.shape[1], wq.shape[0]
    each = tokens // tp // PIECES
    rows, wide = tp * each, _fit(d, 512)

    def body(dq_ref, dk_ref, dv_ref, wq_ref, wk_ref, wv_ref, o_ref):
        left = jnp.concatenate([dq_ref[...].reshape(rows, nq), dk_ref[...].reshape(rows, nk), dv_ref[...].reshape(rows, nk)], axis=1)
        o_ref[...] = nt(left, jnp.concatenate([wq_ref[...], wk_ref[...], wv_ref[...]], axis=1)).astype(BF16)

    part = lambda m: pl.BlockSpec((tp, None, each, m), lambda j: (0, piece, 0, 0))
    w = lambda m: pl.BlockSpec((wide, m), lambda j: (j, 0))
    split = lambda t: t.reshape(tp, PIECES, each, t.shape[1])
    return run(body, (d // wide,), [part(nq), part(nk), part(nk), w(nq), w(nk), w(nk)], [pl.BlockSpec((rows, wide), lambda j: (0, j))],
               [((rows, d), BF16)], (split(dq), split(dk), split(dv), wq, wk, wv), 2 * rows * d * (nq + 2 * nk))[0]


def by_qkv(a, dq, dk, dv):
    tokens, d = a.shape
    nq, nk = dq.shape[1], dk.shape[1]
    tall = _fit(d, 512)

    def body(a_ref, dq_ref, dk_ref, dv_ref, oq_ref, ok_ref, ov_ref):
        turn = a_ref[...].T
        oq_ref[...] = nn(turn, dq_ref[...]).astype(BF16)
        both = nn(turn, jnp.concatenate([dk_ref[...], dv_ref[...]], axis=1)).astype(BF16)
        ok_ref[...], ov_ref[...] = both[:, :nk], both[:, nk:]

    out = lambda m: pl.BlockSpec((tall, m), lambda i: (i, 0))
    return run(body, (d // tall,), [pl.BlockSpec((tokens, tall), lambda i: (0, i)), whole(tokens, nq), whole(tokens, nk), whole(tokens, nk)],
               [out(nq), out(nk), out(nk)], [((d, m), BF16) for m in (nq, nk, nk)], (a, dq, dk, dv), 2 * tokens * d * (nq + 2 * nk))


def gather(t):
    return lax.all_gather(t, "tp", axis=0, tiled=True)


def scatter(t):
    return lax.psum_scatter(t, "tp", scatter_dimension=0, tiled=True)


def layer(tp, x, dy, wq, wk, wv, wo, wg, wu, wd):
    own = x.shape[0]
    pieces = range(PIECES)
    cos, sin = tables(own * tp)

    a = gather(normed(x))
    all_dy = gather(dy)
    q, k, v = qkv(a, wq, wk, wv, cos, sin)
    heads, lse = attend(q, k, v)
    terms = [scatter(projected(heads, wo, tp, c)) for c in pieces]
    h, b = zip(*(added(x, t, c) for c, t in enumerate(terms)))
    b = [gather(t) for t in b]
    dhid = by_hidden(all_dy, wd)
    hid, dg, du, dh, all_dh = [], [], [], [], []
    for c in pieces:
        got = gated(b[c], wg, wu, dhid, tp, c)
        for to, t in zip((hid, dg, du), got):
            to.append(t)
        db = scatter(by_normed(got[1], got[2], wg, wu))
        dh.append(by_states(dy, h[c], db, c))
        all_dh.append(gather(dh[c]))
    d_wg = by_columns(b, dg)
    d_wu = by_columns(b, du)
    d_wd = by_down(hid, all_dy, tp)
    do = by_heads(all_dh, wo, heads.shape[0], tp)
    d_wo = by_wo(heads, all_dh, tp)
    dq, dk, dv = attend_back(q, k, v, do, heads, lse, cos, sin)
    da = [scatter(by_input(dq, dk, dv, wq, wk, wv, tp, c)) for c in pieces]
    d_wq, d_wk, d_wv = by_qkv(a, dq, dk, dv)
    return by_x(dh, x, da), d_wq, d_wk, d_wv, d_wo, d_wg, d_wu, d_wd


def solution(mesh):
    tp = mesh.shape["tp"]

    def step(x, dy, *weights):
        dx, *by_weights = layer(tp, x[0], dy[0], *weights)
        return (dx[None], *by_weights)

    states, by_columns, by_rows = P("dp", "tp", None), P(None, "tp"), P("tp", None)
    weights = (by_columns, by_columns, by_columns, by_rows, by_columns, by_columns, by_rows)
    own = tuple(P("dp", "tp") if spec == by_columns else P(("dp", "tp"), None) for spec in weights)
    return jax.shard_map(step, mesh=mesh, in_specs=(states, states, *weights), out_specs=(states, *own), check_vma=False)
```
